32 devices in a mesh: rep: 2 (over z, core), dp: 16 (over x, y).
Axes of the slice: x: 4, y: 4, z: 1, core: 2. Of those that a mesh axis runs over, the one named last changes fastest.
The devices are a block of a 4x4x8 slice.
Arguments:
- x: bfloat16 [32, 2048, 640], P(('rep', 'dp')), parts along dimension 0
- dy: bfloat16 [32, 2048, 640], P(('rep', 'dp')), parts along dimension 0
- wq: bfloat16 [2, 640, 640], P(None, 'dp')
- wk: bfloat16 [2, 640, 640], P(None, 'dp')
- wv: bfloat16 [2, 640, 640], P(None, 'dp')
- wo: bfloat16 [2, 640, 640], P(None, 'dp')
- w_gate: bfloat16 [2, 640, 2560], P(None, 'dp')
- w_up: bfloat16 [2, 640, 2560], P(None, 'dp')
- w_down: bfloat16 [2, 2560, 640], P(None, 'dp')
- m_wq: float32 [2, 640, 640], P(None, 'dp')
- m_wk: float32 [2, 640, 640], P(None, 'dp')
- m_wv: float32 [2, 640, 640], P(None, 'dp')
- m_wo: float32 [2, 640, 640], P(None, 'dp')
- m_w_gate: float32 [2, 640, 2560], P(None, 'dp')
- m_w_up: float32 [2, 640, 2560], P(None, 'dp')
- m_w_down: float32 [2, 2560, 640], P(None, 'dp')
- v_wq: float32 [2, 640, 640], P(None, 'dp')
- v_wk: float32 [2, 640, 640], P(None, 'dp')
- v_wv: float32 [2, 640, 640], P(None, 'dp')
- v_wo: float32 [2, 640, 640], P(None, 'dp')
- v_w_gate: float32 [2, 640, 2560], P(None, 'dp')
- v_w_up: float32 [2, 640, 2560], P(None, 'dp')
- v_w_down: float32 [2, 2560, 640], P(None, 'dp')
Outputs:
- output 1: bfloat16 [4, 640, 640], P('rep', 'dp'), parts along dimension 0
- output 2: bfloat16 [4, 640, 640], P('rep', 'dp'), parts along dimension 0
- output 3: bfloat16 [4, 640, 640], P('rep', 'dp'), parts along dimension 0
- output 4: bfloat16 [4, 640, 640], P('rep', 'dp'), parts along dimension 0
- output 5: bfloat16 [4, 640, 2560], P('rep', 'dp'), parts along dimension 0
- output 6: bfloat16 [4, 640, 2560], P('rep', 'dp'), parts along dimension 0
- output 7: bfloat16 [4, 2560, 640], P('rep', 'dp'), parts along dimension 0
- output 8: float32 [4, 640, 640], P('rep', 'dp'), parts along dimension 0
- output 9: float32 [4, 640, 640], P('rep', 'dp'), parts along dimension 0
- output 10: float32 [4, 640, 640], P('rep', 'dp'), parts along dimension 0
- output 11: float32 [4, 640, 640], P('rep', 'dp'), parts along dimension 0
- output 12: float32 [4, 640, 2560], P('rep', 'dp'), parts along dimension 0
- output 13: float32 [4, 640, 2560], P('rep', 'dp'), parts along dimension 0
- output 14: float32 [4, 2560, 640], P('rep', 'dp'), parts along dimension 0
- output 15: float32 [4, 640, 640], P('rep', 'dp'), parts along dimension 0
- output 16: float32 [4, 640, 640], P('rep', 'dp'), parts along dimension 0
- output 17: float32 [4, 640, 640], P('rep', 'dp'), parts along dimension 0
- output 18: float32 [4, 640, 640], P('rep', 'dp'), parts along dimension 0
- output 19: float32 [4, 640, 2560], P('rep', 'dp'), parts along dimension 0
- output 20: float32 [4, 640, 2560], P('rep', 'dp'), parts along dimension 0
- output 21: float32 [4, 2560, 640], P('rep', 'dp'), parts along dimension 0
There are 2 independent parts. The reference program is written for one: setup_inputs(seed, part) draws one part's arguments, and reference() takes and returns one part's arrays. A program takes and returns all parts, laid end to end along the dimension named above; an argument that names none is the same for every part.
All inputs are finite; a program needn't handle non-finite values.
Results may differ from the reference program's by a relative error of at most 0.024.
Values are sent between devices in bfloat16 or wider.
A program may use at most 768 MiB of HBM per device.

```python
import jax
import jax.numpy as jnp
from jax import lax

SEQUENCES = 16
TOKENS = 2048
D = 640
HEADS = 5
KV_HEADS = 5
HEAD = 128
FF = 2560
LAYERS = 2
THETA = 10000
NAMES = ("wq", "wk", "wv", "wo", "w_gate", "w_up", "w_down")
SHAPES = {
    "wq": (LAYERS, D, HEADS * HEAD),
    "wk": (LAYERS, D, KV_HEADS * HEAD),
    "wv": (LAYERS, D, KV_HEADS * HEAD),
    "wo": (LAYERS, HEADS * HEAD, D),
    "w_gate": (LAYERS, D, FF),
    "w_up": (LAYERS, D, FF),
    "w_down": (LAYERS, FF, D),
}


def bump(key, n, height):
    away = (jnp.arange(n, dtype=jnp.int32) - jax.random.randint(key, (), 0, n, jnp.int32)) % n
    return jnp.where(away < n // 8, height, 1.0)


def together(key, own, strength):
    shared = jax.random.normal(key, own.shape[1:], jnp.float32)
    return (own + strength * shared) * lax.rsqrt(1 + strength * strength)


def setup_inputs(seed: int = 0, part: int = 0) -> dict:
    kx, kdy, ka, kb, kz, kf, kh, kl, *keys = jax.random.split(jax.random.key(seed), 8 + 3 * len(NAMES))
    kx, kdy, ka, kb = (jax.random.fold_in(k, part) for k in (kx, kdy, ka, kb))
    kw, km, kv = (keys[i::3] for i in range(3))
    shape = (SEQUENCES, TOKENS, D)
    much_x, much_dy = jax.random.uniform(kz, (2,), jnp.float32, 0.0, 1.0)
    loud = 2.0 ** jax.random.uniform(jax.random.fold_in(kz, 1), (), jnp.float32, -1.0, 2.0)
    layers = 2.0 ** jax.random.uniform(kl, (LAYERS, 1, 1), jnp.float32, -1.0, 1.0)
    times = {"wq": 1.0, "wk": 1.0, "wv": 2.0, "wo": layers, "w_gate": 1.0, "w_up": bump(kh, FF, 4.0), "w_down": layers}
    x = together(ka, jax.random.normal(kx, shape, jnp.float32), much_x) * bump(kf, D, 4.0)
    dy = together(kb, jax.random.normal(kdy, shape, jnp.float32), much_dy)
    drawn = {"x": x.astype(jnp.bfloat16), "dy": (loud * dy * (SEQUENCES * TOKENS) ** -0.5).astype(jnp.bfloat16)}
    for key, name in zip(kw, NAMES, strict=True):
        drawn[name] = (jax.random.normal(key, SHAPES[name], jnp.float32) * SHAPES[name][1] ** -0.5 * times[name]).astype(jnp.bfloat16)
    for key, name in zip(km, NAMES, strict=True):
        drawn[f"m_{name}"] = 0.1 * jax.random.normal(key, SHAPES[name], jnp.float32)
    for key, name in zip(kv, NAMES, strict=True):
        drawn[f"v_{name}"] = loud * loud * jax.random.uniform(key, SHAPES[name], jnp.float32, 0.2, 0.6)
    return drawn


def matmul(a, w):
    return jnp.dot(a, w, preferred_element_type=jnp.float32).astype(jnp.bfloat16)


def normed(h):
    wide = h.astype(jnp.float32)
    scale = lax.rsqrt(jnp.mean(wide**2, -1, keepdims=True) + 1e-6)
    return (wide * scale).astype(jnp.bfloat16)


def turned(t, theta):
    half = t.shape[-1] // 2
    angle = jnp.arange(t.shape[0], dtype=jnp.float32)[:, None] * theta ** (-jnp.arange(half, dtype=jnp.float32) / half)
    cos, sin = jnp.cos(angle)[:, None], jnp.sin(angle)[:, None]
    a, b = t[..., :half].astype(jnp.float32), t[..., half:].astype(jnp.float32)
    return jnp.concatenate([a * cos - b * sin, b * cos + a * sin], -1).astype(jnp.bfloat16)


def seen_by(q, k, v):
    tokens, kv = q.shape[0], k.shape[1]
    q = q.reshape(tokens, kv, -1, q.shape[-1])
    scores = jnp.einsum("tgsd,ugd->gstu", q.astype(jnp.float32), k.astype(jnp.float32)) * q.shape[-1] ** -0.5
    place = jnp.arange(tokens)
    weights = jax.nn.softmax(jnp.where(place[:, None] >= place, scores, -jnp.inf), -1).astype(jnp.bfloat16)
    return jnp.einsum("gstu,ugd->tgsd", weights.astype(jnp.float32), v.astype(jnp.float32)).astype(jnp.bfloat16).reshape(tokens, -1)


def layer(h, w):
    a = normed(h)
    q, k = (turned(matmul(a, w[name]).reshape(h.shape[0], -1, HEAD), THETA) for name in ("wq", "wk"))
    h = h + matmul(seen_by(q, k, matmul(a, w["wv"]).reshape(h.shape[0], -1, HEAD)), w["wo"])
    b = normed(h)
    gate = jnp.dot(b, w["w_gate"], preferred_element_type=jnp.float32)
    up = jnp.dot(b, w["w_up"], preferred_element_type=jnp.float32)
    return h + matmul((jax.nn.silu(gate) * up).astype(jnp.bfloat16), w["w_down"])


def adamw(w, m, v, g):
    m = 0.9 * m + 0.1 * g
    v = 0.95 * v + 0.05 * g * g
    step = m * lax.rsqrt(v + 1e-8) + 0.1 * w
    return (w - 0.02 * step).astype(jnp.bfloat16), m, v


def stack(weights, h):
    return lax.scan(lambda h, w: (layer(h, w), None), h, weights)[0]


def reference(x, dy, wq, wk, wv, wo, w_gate, w_up, w_down, m_wq, m_wk, m_wv, m_wo, m_w_gate, m_w_up, m_w_down, v_wq, v_wk, v_wv, v_wo, v_w_gate, v_w_up, v_w_down):
    weights = dict(zip(NAMES, (wq, wk, wv, wo, w_gate, w_up, w_down), strict=True))

    def take(so_far, sequence):
        h, by_y = sequence
        _, back = jax.vjp(stack, weights, h)
        by_weights, by_h = back(by_y)
        return jax.tree.map(lambda total, term: total + term.astype(jnp.float32), so_far, by_weights), by_h

    none_yet = {name: jnp.zeros(w.shape, jnp.float32) for name, w in weights.items()}
    by_weights, by_x = lax.scan(take, none_yet, (x, dy))
    gradients = [by_weights[name].astype(jnp.bfloat16).astype(jnp.float32) for name in NAMES]
    first = (m_wq, m_wk, m_wv, m_wo, m_w_gate, m_w_up, m_w_down)
    second = (v_wq, v_wk, v_wv, v_wo, v_w_gate, v_w_up, v_w_down)
    new = [adamw(weights[name].astype(jnp.float32), m, v, g) for name, m, v, g in zip(NAMES, first, second, gradients, strict=True)]
    return tuple(one[which] for which in range(3) for one in new)
```

```python
import jax
import jax.numpy as jnp
from jax import lax
from jax.experimental import pallas as pl
from jax.experimental.pallas import tpu as pltpu

NEG = -1e30
HIDDEN = 2 * NEG
LOG2E = 1.4426950408889634
VMEM = 56 * 2**20
BLOCK = 512


def _dot(a, b, ca, cb):
    return lax.dot_general(a, b, (((ca,), (cb,)), ((), ())), preferred_element_type=jnp.float32)


def _visible():
    return lax.broadcasted_iota(jnp.int32, (BLOCK, BLOCK), 1) >= lax.broadcasted_iota(jnp.int32, (BLOCK, BLOCK), 0)


def _forward(q_ref, k_ref, v_ref, o_ref, lse_ref, top_s, mix_s):
    heads, d = q_ref.shape[0], q_ref.shape[2]
    scale = d**-0.5
    e = scale * LOG2E
    top_s[...] = jnp.full(top_s.shape, NEG, jnp.float32)
    mix_s[...] = jnp.zeros(mix_s.shape, jnp.float32)
    ones = jnp.ones((8, BLOCK), k_ref.dtype)

    def block(j, masked):
        here = pl.ds(pl.multiple_of(j * BLOCK, BLOCK), BLOCK)
        scores = [_dot(k_ref[i, here, :], q_ref[i], 1, 1) for i in range(heads)]
        ok = _visible() if masked else None
        weights, keeps = [], []
        for i, s in enumerate(scores):
            if masked:
                s = jnp.where(ok, s, HIDDEN)
            old = top_s[i : i + 1, :]
            top = jnp.maximum(old, s.max(axis=0, keepdims=True))
            top_s[i : i + 1, :] = top
            weights.append(jnp.exp2((s - top) * e).astype(k_ref.dtype))
            keeps.append(jnp.exp2((old - top) * e))
        for i, (p, keep) in enumerate(zip(weights, keeps)):
            values = jnp.concatenate([v_ref[i, here, :].T, ones], axis=0)
            mix_s[i] = mix_s[i] * keep + _dot(values, p, 1, 0)

    n = pl.program_id(0)
    lax.fori_loop(0, n, lambda j, _: block(j, False), None)
    block(n, True)
    for i in range(heads):
        total = mix_s[i, d : d + 1, :]
        o_ref[i] = (mix_s[i, :d, :] * (1 / total)).T.astype(o_ref.dtype)
        lse_ref[i : i + 1, :] = top_s[i : i + 1, :] * scale + jnp.log(total)


def attend(q, k, v):
    h, t, d = q.shape
    block, stats = pl.BlockSpec((h, BLOCK, d), lambda n: (0, n, 0)), pl.BlockSpec((h, BLOCK), lambda n: (0, n))
    whole = pl.BlockSpec((h, t, d), lambda n: (0, 0, 0))
    return pl.pallas_call(
        _forward,
        grid=(t // BLOCK,),
        in_specs=[block, whole, whole],
        out_specs=[block, stats],
        scratch_shapes=[pltpu.VMEM((h, BLOCK), jnp.float32), pltpu.VMEM((h, d + 8, BLOCK), jnp.float32)],
        out_shape=[jax.ShapeDtypeStruct((h, t, d), q.dtype), jax.ShapeDtypeStruct((h, t), jnp.float32)],
        compiler_params=pltpu.CompilerParams(dimension_semantics=("arbitrary",), vmem_limit_bytes=VMEM),
        cost_estimate=pl.CostEstimate(flops=4 * h * t * t * d, transcendentals=h * t * t, bytes_accessed=8 * h * t * d),
    )(q, k, v)


def row_dot(d_out, out):
    return (d_out.astype(jnp.float32) * out.astype(jnp.float32)).sum(-1)


def _backward(q_ref, k_ref, v_ref, do_ref, lse_ref, delta_ref, *rest):
    dq_ref, dk_ref, dv_ref, dq_s, dk_s, dv_s = rest[-6:]
    heads, low, scale = q_ref.shape[0], q_ref.dtype, q_ref.shape[2] ** -0.5
    n = pl.program_id(0)
    e = scale * LOG2E

    @pl.when(n == 0)
    def _():
        dk_s[...] = jnp.zeros_like(dk_s)
        dv_s[...] = jnp.zeros_like(dv_s)

    dq_s[...] = jnp.zeros_like(dq_s)

    def block(j, masked):
        here = pl.ds(pl.multiple_of(j * BLOCK, BLOCK), BLOCK)
        scores = [_dot(k_ref[i, here, :], q_ref[i], 1, 1) for i in range(heads)]
        dps = [_dot(v_ref[i, here, :], do_ref[i], 1, 1) for i in range(heads)]
        ok = _visible() if masked else None
        for i in range(heads):
            p = jnp.exp2(scores[i] * e - lse_ref[i : i + 1, :] * LOG2E)
            if masked:
                p = jnp.where(ok, p, 0.0)
            ds = (p * (dps[i] - delta_ref[i : i + 1, :])).astype(low)
            dv_s[i, here, :] += _dot(p.astype(low), do_ref[i], 1, 0)
            dk_s[i, here, :] += _dot(ds, q_ref[i], 1, 0)
            dq_s[i] += _dot(k_ref[i, here, :].T, ds, 1, 0)

    lax.fori_loop(0, n, lambda j, _: block(j, False), None)
    block(n, True)
    for i in range(heads):
        dq_ref[i] = (dq_s[i] * scale).T.astype(dq_ref.dtype)

    @pl.when(n == pl.num_programs(0) - 1)
    def _():
        dk_ref[...] = (dk_s[...] * scale).astype(dk_ref.dtype)
        dv_ref[...] = dv_s[...].astype(dv_ref.dtype)


def attend_bwd(q, k, v, d_out, lse, delta, after=()):
    h, t, d = q.shape
    block, stats = pl.BlockSpec((h, BLOCK, d), lambda n: (0, n, 0)), pl.BlockSpec((h, BLOCK), lambda n: (0, n))
    whole = pl.BlockSpec((h, t, d), lambda n: (0, 0, 0))
    one = jax.ShapeDtypeStruct((h, t, d), q.dtype)
    return pl.pallas_call(
        _backward,
        grid=(t // BLOCK,),
        in_specs=[block, whole, whole, block, stats, stats] + [pl.BlockSpec(memory_space=pl.ANY)] * len(after),
        out_specs=[block, whole, whole],
        scratch_shapes=[pltpu.VMEM((h, d, BLOCK), jnp.float32), pltpu.VMEM((h, t, d), jnp.float32), pltpu.VMEM((h, t, d), jnp.float32)],
        out_shape=[one] * 3,
        compiler_params=pltpu.CompilerParams(dimension_semantics=("arbitrary",), vmem_limit_bytes=VMEM),
        cost_estimate=pl.CostEstimate(flops=10 * h * t * t * d, transcendentals=h * t * t, bytes_accessed=14 * h * t * d),
    )(q, k, v, d_out, lse, delta, *after)


from jax.sharding import PartitionSpec as P

HEAD = 128
THETA = 10000
NAMES = ("wq", "wk", "wv", "wo", "w_gate", "w_up", "w_down")
F32, BF16 = jnp.float32, jnp.bfloat16
ROWS = 512
WIDE = 512


def normed(h):
    wide = h.astype(F32)
    scale = lax.rsqrt(jnp.mean(wide**2, -1, keepdims=True) + 1e-6)
    return (wide * scale).astype(BF16)


def normed_back(h, by):
    wide = h.astype(F32)
    scale = lax.rsqrt(jnp.mean(wide**2, -1, keepdims=True) + 1e-6)
    by = by.astype(BF16).astype(F32)
    inner = jnp.mean(by * wide, -1, keepdims=True)
    return (scale * by - wide * (inner * scale * scale * scale)).astype(BF16)


def added(a, b):
    return (a.astype(F32) + b.astype(F32)).astype(BF16)


def beside(ref):
    return jnp.concatenate([ref[i] for i in range(ref.shape[0])], axis=1)


def swapped(t):
    return jnp.concatenate([t[:, HEAD // 2 :], t[:, : HEAD // 2]], axis=1)


def call(body, grid, ins, outs, given, scratch=(), flops=0, after=()):
    spec = lambda s: pl.BlockSpec(s[0], s[1])

    def kernel(*refs):
        body(*refs[: len(given)], *refs[len(given) + len(after) :])

    return pl.pallas_call(
        kernel,
        grid=grid,
        in_specs=[spec(s) for s in ins] + [pl.BlockSpec(memory_space=pl.ANY)] * len(after),
        out_specs=[spec(s) for s in outs],
        out_shape=[jax.ShapeDtypeStruct(s[2], s[3]) for s in outs],
        scratch_shapes=list(scratch),
        compiler_params=pltpu.CompilerParams(dimension_semantics=("arbitrary",) * len(grid), vmem_limit_bytes=VMEM),
        cost_estimate=pl.CostEstimate(flops=flops, transcendentals=0, bytes_accessed=sum(a.size * a.dtype.itemsize for a in given)),
    )(*given, *after)


def project(h, qk, vo, cos, sin):
    t, d = h.shape
    heads = d // HEAD

    def body(h_ref, qk_ref, v_ref, cos_ref, sin_ref, q_out, k_out, v_out):
        a = normed(h_ref[...])
        both = _dot(a, qk_ref[...], 1, 0).astype(BF16)
        v = _dot(a, v_ref[...], 1, 0).astype(BF16)
        c, s = cos_ref[...], sin_ref[...]
        for i in range(heads):
            for out, at in ((q_out, i), (k_out, heads + i)):
                one = both[:, at * HEAD : (at + 1) * HEAD].astype(F32)
                out[i] = (one * c + swapped(one) * s).astype(BF16)
            v_out[i] = v[:, i * HEAD : (i + 1) * HEAD]

    row, whole = lambda i: (i, 0), lambda i: (0, 0)
    out = ((heads, ROWS, HEAD), lambda i: (0, i, 0), (heads, t, HEAD), BF16)
    return call(body, (t // ROWS,), [((ROWS, d), row), ((d, 2 * d), whole), ((d, d), whole), ((ROWS, HEAD), row), ((ROWS, HEAD), row)],
                [out] * 3, [h, qk, vo, cos, sin], flops=6 * t * d * d)


def project_back(h, by_h, by_q, by_k, by_v, qk, vo, cos, sin, more, after):
    t, d = h.shape
    heads = d // HEAD
    last = t // ROWS - 1

    def body(h_ref, by_ref, q_ref, k_ref, v_ref, qk_ref, wv_ref, cos_ref, sin_ref, w_out, *rest):
        i, total = pl.program_id(0), rest[-1]

        @pl.when(i == 0)
        def _():
            total[...] = jnp.zeros_like(total)

        h = h_ref[...]
        a = normed(h)
        c, s = cos_ref[...], sin_ref[...]
        turned_back = lambda x: (x * c + swapped(x * s)).astype(BF16)
        parts = [turned_back(ref[n].astype(F32)) for ref in (q_ref, k_ref) for n in range(heads)]
        both, by_v = jnp.concatenate(parts, axis=1), beside(v_ref)
        at = a.T
        total[:, : 2 * d] += _dot(at, both, 1, 0)
        total[:, 2 * d :] += _dot(at, by_v, 1, 0)
        if more:
            by_a = _dot(both, qk_ref[...], 1, 1) + _dot(by_v, wv_ref[...], 1, 1)
            rest[0][...] = added(by_ref[...], normed_back(h, by_a))

        @pl.when(i == last)
        def _():
            w_out[...] = total[...].astype(BF16)

    row, whole, part = lambda i: (i, 0), lambda i: (0, 0), ((heads, ROWS, HEAD), lambda i: (0, i, 0))
    outs = [((d, 3 * d), whole, (d, 3 * d), BF16)] + [((ROWS, d), row, (t, d), BF16)] * more
    got = call(body, (t // ROWS,),
               [((ROWS, d), row), ((ROWS, d), row), part, part, part, ((d, 2 * d), whole), ((d, d), whole), ((ROWS, HEAD), row), ((ROWS, HEAD), row)],
               outs, [h, by_h, by_q, by_k, by_v, qk, vo, cos, sin], [pltpu.VMEM((d, 3 * d), F32)], (6 + 6 * more) * t * d * d, after)
    return got if more else (got[0], None)


def output(h, o, vo):
    t, d = h.shape

    def body(h_ref, o_ref, w_ref, out):
        out[...] = added(h_ref[...], _dot(beside(o_ref), w_ref[...], 1, 0).astype(BF16))

    row = lambda i: (i, 0)
    return call(body, (t // ROWS,), [((ROWS, d), row), ((d // HEAD, ROWS, HEAD), lambda i: (0, i, 0)), ((d, d), lambda i: (0, 1))],
                [((ROWS, d), row, (t, d), BF16)], [h, o, vo], flops=2 * t * d * d)[0]


def output_back(by, o, vo, after):
    t, d = by.shape
    heads = d // HEAD
    last = t // ROWS - 1

    def body(by_ref, o_ref, w_ref, o_out, w_out, total):
        i = pl.program_id(0)

        @pl.when(i == 0)
        def _():
            total[...] = jnp.zeros_like(total)

        by = by_ref[...]
        by_o = _dot(by, w_ref[...], 1, 1).astype(BF16)
        for n in range(heads):
            o_out[n] = by_o[:, n * HEAD : (n + 1) * HEAD]
        total[...] += _dot(beside(o_ref).T, by, 1, 0)

        @pl.when(i == last)
        def _():
            w_out[...] = total[...].astype(BF16)

    row, part = lambda i: (i, 0), ((heads, ROWS, HEAD), lambda i: (0, i, 0))
    return call(body, (t // ROWS,), [((ROWS, d), row), part, ((d, d), lambda i: (0, 1))],
                [(*part, (heads, t, HEAD), BF16), ((d, d), lambda i: (0, 0), (d, d), BF16)], [by, o, vo], [pltpu.VMEM((d, d), F32)], 4 * t * d * d, after)


def ffn(h, gate, up, down):
    t, d = h.shape
    ff = gate.shape[1]

    def body(h_ref, gate_ref, up_ref, down_ref, out):
        h = h_ref[...]
        b = normed(h)
        total = jnp.zeros(h.shape, F32)
        for at in range(0, ff, WIDE):
            g, u = _dot(b, gate_ref[:, at : at + WIDE], 1, 0), _dot(b, up_ref[:, at : at + WIDE], 1, 0)
            total += _dot((g * jax.nn.sigmoid(g) * u).astype(BF16), down_ref[at : at + WIDE, :], 1, 0)
        out[...] = added(h, total.astype(BF16))

    row, whole = lambda i: (i, 0), lambda i: (0, 0)
    return call(body, (t // ROWS,), [((ROWS, d), row), ((d, ff), whole), ((d, ff), whole), ((ff, d), whole)],
                [((ROWS, d), row, (t, d), BF16)], [h, gate, up, down], flops=6 * t * d * ff)[0]


def ffn_back(h, by, gate, up, down, after):
    t, d = h.shape
    ff = gate.shape[1]
    last = ff // WIDE - 1

    def body(h_ref, by_ref, gate_ref, up_ref, down_ref, h_out, gate_out, up_out, down_out, b_s, bt_s, byt_s, act_s, dg_s, du_s, db_s):
        c = pl.program_id(0)

        @pl.when(c == 0)
        def _():
            for at in range(0, t, ROWS):
                b = normed(h_ref[at : at + ROWS, :])
                b_s[at : at + ROWS, :] = b
                bt_s[:, at : at + ROWS] = b.T
                byt_s[:, at : at + ROWS] = by_ref[at : at + ROWS, :].T
            db_s[...] = jnp.zeros_like(db_s)

        def block(n, _):
            here = pl.ds(pl.multiple_of(n * ROWS, ROWS), ROWS)
            b = b_s[here, :]
            g, u = _dot(b, gate_ref[...], 1, 0), _dot(b, up_ref[...], 1, 0)
            by_act = _dot(by_ref[here, :], down_ref[...], 1, 1).astype(BF16).astype(F32)
            s = jax.nn.sigmoid(g)
            gs = g * s
            act_s[here, :] = (gs * u).astype(BF16)
            du = (by_act * gs).astype(BF16)
            dg = (by_act * u * (s + gs * (1.0 - s))).astype(BF16)
            du_s[here, :] = du
            dg_s[here, :] = dg
            db_s[here, :] += _dot(dg, gate_ref[...], 1, 1) + _dot(du, up_ref[...], 1, 1)

        lax.fori_loop(0, t // ROWS, block, None)
        gate_out[...] = _dot(bt_s[...], dg_s[...], 1, 0).astype(BF16)
        up_out[...] = _dot(bt_s[...], du_s[...], 1, 0).astype(BF16)
        down_out[...] = _dot(byt_s[...], act_s[...], 1, 0).T.astype(BF16)

        @pl.when(c == last)
        def _():
            for at in range(0, t, ROWS):
                here = slice(at, at + ROWS)
                h_out[here, :] = added(by_ref[here, :], normed_back(h_ref[here, :], db_s[here, :]))

    whole, across, along = lambda c: (0, 0), ((d, WIDE), lambda c: (0, c)), ((WIDE, d), lambda c: (c, 0))
    tall = pltpu.VMEM((t, WIDE), BF16)
    return call(body, (ff // WIDE,), [((t, d), whole), ((t, d), whole), across, across, along],
                [((t, d), whole, (t, d), BF16), (*across, (d, ff), BF16), (*across, (d, ff), BF16), (*along, (ff, d), BF16)],
                [h, by, gate, up, down],
                [pltpu.VMEM((t, d), BF16), pltpu.VMEM((d, t), BF16), pltpu.VMEM((d, t), BF16), tall, tall, tall, pltpu.VMEM((t, d), F32)],
                16 * t * d * ff, after)


def angles(tokens):
    half = HEAD // 2
    angle = jnp.arange(tokens, dtype=F32)[:, None] * THETA ** (-jnp.arange(half, dtype=F32) / half)
    cos, sin = jnp.cos(angle), jnp.sin(angle)
    return jnp.concatenate([cos, cos], -1), jnp.concatenate([-sin, sin], -1)


def adamw(w, m, v, g):
    m = 0.9 * m + 0.1 * g
    v = 0.95 * v + 0.05 * g * g
    step = m * lax.rsqrt(v + 1e-8) + 0.1 * w
    return (w - 0.02 * step).astype(BF16), m, v


def solution(mesh):
    side = round(mesh.shape["dp"] ** 0.5)
    pairs = [(r, r ^ 1) for r in range(mesh.shape["rep"])]

    def moved(t, axis, by):
        to = lambda x, y: ((x + by) % side) * side + y if axis == 0 else x * side + (y + by) % side
        return lax.ppermute(t, "dp", [(x * side + y, to(x, y)) for x in range(side) for y in range(side)])

    def gathered(mine):
        return lax.all_gather(mine, "dp", axis=0, tiled=True)

    def shared(mine, mine_first):
        other = lax.ppermute(mine, "rep", pairs)
        return jnp.where(mine_first, mine, other), jnp.where(mine_first, other, mine)

    def sent(g, axis):
        at = lax.axis_index("dp")
        place = lax.div(at, side) if axis == 0 else lax.rem(at, side)
        dim = 0 if g.ndim == 3 else axis
        g = g if g.ndim == 3 else g.reshape(side, side, -1, g.shape[-1])
        block = lambda by: lax.dynamic_index_in_dim(g, lax.rem(place + by, side), dim, keepdims=False)
        return [block(0)] + [moved(block(by), axis, by) for by in range(1, side)]

    def joined(parts):
        return sum(p.astype(F32) for p in parts).astype(BF16)

    def parted(t, d):
        return [t[:, :d], t[:, d : 2 * d], t[:, 2 * d :]]

    def scattered(g):
        return lax.psum_scatter(g, "dp", scatter_dimension=0, tiled=True)

    def step(x, dy, *arrays):
        weights, m, v = (arrays[i : i + 7] for i in (0, 7, 14))
        layers, d = weights[0].shape[0], x.shape[2]
        mine_first = lax.rem(lax.axis_index("rep"), 2) == 0
        cos, sin = angles(x.shape[1])

        def halves(number):
            wq, wk, wv, wo, gate, up, down = (w[number] for w in weights)
            rows = wq.shape[0]
            pick = lambda a, b: jnp.where(mine_first, jnp.concatenate(a, 1), jnp.concatenate(b, 1))
            parts = [down[at : at + rows] for at in range(0, down.shape[0], rows)]
            half = len(parts) // 2
            return pick([wq, wk], [wv, wo]), pick([gate, *parts[:half]], [up, *parts[half:]])

        def stacked(a, b):
            blocks, rows = mesh.shape["dp"], a.shape[0] // mesh.shape["dp"]
            return jnp.concatenate([t.reshape(blocks, rows, -1, d).transpose(0, 2, 1, 3) for t in (a, b)], 1).reshape(-1, d)

        ff = weights[4].shape[2]
        of_attention, of_ffn = halves(0)
        arriving = [gathered(of_attention), gathered(of_ffn)]
        h, kept = x[0], []
        for number in range(layers):
            if number + 1 < layers:
                own = [t.shape[1] for t in halves(number + 1)]
                later = gathered(jnp.concatenate(halves(number + 1), 1))
            qk, vo = shared(arriving[0], mine_first)
            q, k, value = project(h, qk, vo, cos, sin)
            o, lse = attend(q, k, value)
            o, rest = lax.optimization_barrier((o, arriving[1]))
            gate, up = shared(rest[:, :ff], mine_first)
            down = stacked(*shared(rest[:, ff:], mine_first))
            middle = output(h, o, vo)
            kept.append((h, qk, vo, gate, up, down, q, k, value, o, lse, middle))
            if number + 1 < layers:
                h = ffn(middle, gate, up, down)
                h, later = lax.optimization_barrier((h, later))
                arriving = [later[:, : own[0]], later[:, own[0] :]]
        tied = lax.optimization_barrier
        cut = 2 * d - 2 * HEAD
        by, mine, flying = dy[0], [None] * layers, []
        for number in reversed(range(layers)):
            h, qk, vo, gate, up, down, q, k, value, o, lse, middle = kept[number]
            by, gate, up, down = ffn_back(middle, by, gate, up, down, ())
            if flying:
                flying, by = tied((flying, by))
                flying = [sent(joined(flying[0]), 1), sent(joined(flying[1]), 0)]
            gate_sum = scattered(gate)
            up_on_its_way = scattered(up) if number == layers - 1 else sent(up, 1)
            by_o, wo = output_back(by, o, vo, ())
            halfway = [sent(down, 0), sent(wo, 1)]
            by_q, by_k, by_v = attend_bwd(q, k, value, by_o, lse, row_dot(by_o, o), (gate, up, down, wo))
            halfway, flying, by_q = tied((halfway, flying, by_q))
            if flying:
                mine[number + 1][:3] = parted(jnp.concatenate([joined(t) for t in flying], 1), d)
            halfway = [sent(joined(halfway[0]), 1), sent(joined(halfway[1]), 0)]
            if number < layers - 1:
                up_on_its_way, by_k = tied((up_on_its_way, by_k))
                up_on_its_way = sent(joined(up_on_its_way), 0)
            qkv, by = project_back(h, by, by_q, by_k, by_v, qk, vo, cos, sin, number > 0, ())
            flying = [sent(qkv[:, :cut], 0), sent(qkv[:, cut:], 1)]
            halfway, qkv = tied((halfway, qkv))
            down_sum, wo_sum = (joined(t) for t in halfway)
            up_sum = up_on_its_way if number == layers - 1 else joined(up_on_its_way)
            mine[number] = [None, None, None, wo_sum, gate_sum, up_sum, down_sum]
        flying = [sent(joined(flying[0]), 1), sent(joined(flying[1]), 0)]
        mine[0][:3] = parted(jnp.concatenate([joined(t) for t in flying], 1), d)
        gradients = [jnp.stack([mine[number][i] for number in range(layers)]).astype(F32) for i in range(7)]
        new = [adamw(w.astype(F32), m, v, g) for w, m, v, g in zip(weights, m, v, gradients, strict=True)]
        return tuple(one[which] for which in range(3) for one in new)

    states, cut = P(("rep", "dp"), None, None), P(None, "dp", None)
    return jax.shard_map(
        step,
        mesh=mesh,
        in_specs=(states, states) + (cut,) * 21,
        out_specs=(P("rep", "dp", None),) * 21,
        check_vma=False,
    )
```
